32 devices in a mesh: gx: 4 (over y, x), gy: 2 (over core), gz: 4 (over z).
Axes of the slice: x: 2, y: 2, z: 4, core: 2. Of those that a mesh axis runs over, the one named last changes fastest.
Arguments:
- potential: float32 [240, 120, 512], P('gx', 'gy', 'gz'), may hold values from -6 to 6
- frag_root: int32 [3, 128], P(None, ('gx', 'gy', 'gz')), may hold values from 0 to 511, as said below
Outputs:
- frag_fields: float32 [128, 110592], P(('gx', 'gy', 'gz'))
The draws below stay inside these ranges and needn't reach their ends.
Inputs may be any that keep to these rules, and one draw needn't show every extreme that they name: `frag_root`: fragment f is held by the device of linear index f // 4 (gx slowest). Along each dimension the box's first cell is the start of a block plus an offset in [-34, B - 34), B being that dimension's cells of one device. Along y and z that block is the holding device's own; along x it is the block of some device with the same gy and gz index, the anchor. Every anchor of a device supplies exactly 1 of its fragments.
All inputs are finite; a program needn't handle non-finite values.
Results may differ from the reference program's by a relative error of at most 0.00007.
Values sent between devices are 32-bit elements; how exact they have to be, the bound alone decides.
A program may use at most 320 MiB of HBM per device.

```python
import math
import jax
import jax.numpy as jnp
from jax import lax

G = 48
CAP = 1
SLOTS = 4
BX = 60
BY = 60
BZ = 128
BOX = 68
HALO = 34
NX = 240
NY = 120
NZ = 512
N_GX = 4
N_GY = 2
N_GZ = 4


def draw_frag_root(key, part):
    subkeys = jax.random.split(jax.random.fold_in(key, 17), 6)
    devices = N_GX * N_GY * N_GZ
    pair_count = SLOTS // CAP
    favour = jax.random.randint(subkeys[0], (N_GX,), 0, 4) * 300
    jitter = jax.random.randint(subkeys[1], (devices, N_GX), 0, 1000)
    scores = (jitter + favour[None, :]) * N_GX + jnp.arange(N_GX, dtype=jnp.int32)[None, :]
    dummy_values, picked = lax.top_k(scores, pair_count)
    listed = jnp.repeat(picked.astype(jnp.int32), CAP, axis=1)
    shuffle_keys = jax.random.randint(subkeys[2], (devices, SLOTS), 0, 1000) * SLOTS + jnp.arange(SLOTS, dtype=jnp.int32)[None, :]
    shuffled = jnp.argsort(shuffle_keys, axis=1)
    anchors = jnp.take_along_axis(listed, shuffled, axis=1).reshape(-1)
    device = jnp.arange(devices * SLOTS, dtype=jnp.int32) // SLOTS
    row_y = device // N_GZ % N_GY
    row_z = device % N_GZ
    lowest = -HALO
    offset_x = jax.random.randint(subkeys[3], (devices * SLOTS,), lowest, BX - HALO)
    offset_y = jax.random.randint(subkeys[4], (devices * SLOTS,), lowest, BY - HALO)
    offset_z = jax.random.randint(subkeys[5], (devices * SLOTS,), lowest, BZ - HALO)
    offset_x = offset_x.at[0].set(lowest).at[1].set(BX - HALO - 1)
    offset_y = offset_y.at[0].set(lowest).at[1].set(BY - HALO - 1)
    offset_z = offset_z.at[0].set(lowest).at[1].set(BZ - HALO - 1)
    root_x = jnp.mod(anchors * BX + offset_x, BX * N_GX)
    root_y = jnp.mod(row_y * BY + offset_y, BY * N_GY)
    root_z = jnp.mod(row_z * BZ + offset_z, BZ * N_GZ)
    return jnp.stack([root_x, root_y, root_z]).astype(jnp.int32)


def steps_of(key, dims, pieces, smallest, top_value):
    level = 1.0
    for dim, shards_of in pieces:
        steps = jax.random.uniform(jax.random.fold_in(jax.random.fold_in(key, 6), dim), (shards_of,), jnp.float32, smallest / len(pieces), top_value / len(pieces))
        level = level * jnp.repeat(jnp.exp(steps), dims[dim] // shards_of).reshape((-1,) + (1,) * (len(dims) - 1 - dim))
    return level


def scatter_about(rng, dims, scale, most, shards=(), kind=jnp.bfloat16):
    array = scale * jax.random.normal(rng, dims, jnp.float32)
    if shards:
        array = array * steps_of(rng, dims, shards, -0.22, 0.18)
    return jnp.clip(array, -most, most).astype(kind)


def setup_inputs(seed: int = 0) -> dict:
    splits = jax.random.split(jax.random.key(seed), 3)
    potential = scatter_about(splits[0], (NX, NY, NZ), 1.0, 6.0, ((0, 4), (1, 2), (2, 4)), jnp.float32)
    frag_root = draw_frag_root(jax.random.fold_in(splits[2], 71), 0)
    return {"potential": potential, "frag_root": frag_root}


def interp_table(points, cells):
    row_index = jnp.arange(points, dtype=jnp.int32)[:, None]
    col_index = jnp.arange(cells, dtype=jnp.int32)[None, :]
    offset = row_index * cells - col_index * points
    period = points * cells
    summed = jnp.ones((points, cells), jnp.float32)
    for harmonic in range(1, points // 2):
        phase_angle = jnp.mod(harmonic * offset, period).astype(jnp.float32)
        summed = summed + 2.0 * jnp.cos((2.0 * math.pi / period) * phase_angle)
    return summed / cells


def refine(window, matrix):
    highest = lax.Precision.HIGHEST
    step_x = jnp.einsum('ax,xyz->ayz', matrix, window, precision=highest)
    step_y = jnp.einsum('by,ayz->abz', matrix, step_x, precision=highest)
    step_z = jnp.einsum('cz,abz->abc', matrix, step_y, precision=highest)
    return step_z.reshape(-1)


def reference(potential, frag_root):
    matrix = interp_table(G, BOX)
    wrapped = jnp.pad(potential, ((0, BOX), (0, BOX), (0, BOX)), mode="wrap")

    def single(corner):
        window = lax.dynamic_slice(wrapped, (corner[0], corner[1], corner[2]), (BOX, BOX, BOX))
        return refine(window, matrix)

    return lax.map(single, frag_root.T.astype(jnp.int32))
```

```python
import math

import jax
import jax.numpy as jnp
from jax import lax
from jax.sharding import PartitionSpec as P

G = 48
BOX = 68
HALO = 34
HIGH = lax.Precision.HIGH


def shift(array, axis, step):
    devices = lax.axis_size(axis)
    return lax.ppermute(array, axis, [(i, (i + step) % devices) for i in range(devices)])


def placed(start, cells, period, valid):
    place = jnp.mod(cells - start[..., None], period)
    inside = jnp.logical_and(place < BOX, valid[..., None])
    base = interp_values()
    index = jnp.where(inside, place, BOX)
    hot = (index[..., None, :] == jnp.arange(BOX, dtype=jnp.int32)[:, None]).astype(jnp.float32)
    return jnp.einsum("ax,...xe->...ae", base, hot, precision=lax.Precision.HIGHEST)


def interp_values():
    row_index = jnp.arange(G, dtype=jnp.int32)[:, None]
    col_index = jnp.arange(BOX, dtype=jnp.int32)[None, :]
    offset = row_index * BOX - col_index * G
    period = G * BOX
    summed = jnp.ones((G, BOX), jnp.float32)
    for harmonic in range(1, G // 2):
        phase_angle = jnp.mod(harmonic * offset, period).astype(jnp.float32)
        summed = summed + 2.0 * jnp.cos(2.0 * math.pi / period * phase_angle)
    return summed / BOX


def body(potential, frag_root):
    bx, by, bz = potential.shape
    n = lax.axis_size("gx")
    ny = lax.axis_size("gy")
    nz = lax.axis_size("gz")
    ix, iy, iz = lax.axis_index("gx"), lax.axis_index("gy"), lax.axis_index("gz")
    total_x, total_y, total_z = bx * n, by * ny, bz * nz
    slots = frag_root.shape[1]

    roots = [frag_root] + [shift(frag_root, "gx", j) for j in range(1, n)]
    low = shift(potential[:, :, bz - HALO:].transpose(2, 0, 1).reshape(HALO, bx * by), "gz", 1)
    high = shift(potential[:, :, :HALO].transpose(2, 0, 1).reshape(HALO, bx * by), "gz", -1)
    own = [potential] + [shift(potential, "gy", -j) for j in range(1, ny)]
    lows = [low] + [shift(low, "gy", -j) for j in range(1, ny)]
    highs = [high] + [shift(high, "gy", -j) for j in range(1, ny)]

    def joined(l, o, h):
        back = lambda v: v.reshape(HALO, bx, by).transpose(1, 2, 0)
        return jnp.concatenate([back(l), o, back(h)], axis=2)

    circle = jnp.concatenate([joined(*t) for t in zip(lows, own, highs)], axis=1)

    root = jnp.stack(roots)
    anchor = jnp.mod(root[:, 0] + HALO, total_x) // bx
    start_y = jnp.mod(root[:, 1] - iy * by, total_y)
    start_z = jnp.mod(root[:, 2] + HALO - iz * bz, total_z)
    cells_y = jnp.arange(total_y, dtype=jnp.int32)
    cells_z = jnp.arange(bz + 2 * HALO, dtype=jnp.int32)
    parts = []
    for delta, rows in ((1, slice(bx - HALO, bx)), (0, slice(0, bx)), (-1, slice(0, HALO))):
        hit = anchor == jnp.mod(ix + delta, n)
        valid = jnp.any(hit, axis=1)
        pick = lambda v: jnp.sum(jnp.where(hit, v, 0), axis=1)
        my = placed(pick(start_y), cells_y, total_y, valid)
        mz = placed(pick(start_z), cells_z, 1 << 20, valid)
        u = jnp.einsum("xyz,hcz->hcxy", circle[rows], mz, precision=HIGH)
        v = jnp.einsum("hcxy,hby->hxbc", u, my, precision=HIGH)
        parts.append(v.reshape(n, -1, G * G))
    sent = jnp.concatenate(parts, axis=1)
    got = [sent[0]] + [shift(sent[j], "gx", -j) for j in range(1, n)]
    got = jnp.stack(got)

    mine = jnp.mod(frag_root[0] + HALO, total_x)
    slab = mine // bx
    rel = mine - slab * bx
    width = bx + 2 * HALO
    mx = placed(rel, jnp.arange(width, dtype=jnp.int32), 1 << 20, jnp.ones((slots,), bool))

    def one(k):
        j = jnp.mod(slab[k] - ix, n)
        before = jnp.mod(j - 1, n)
        after = jnp.mod(j + 1, n)
        piece = lambda b, lo, hi: lax.dynamic_slice(got, (b, lo, 0), (1, hi - lo, G * G))[0]
        rows = jnp.concatenate([
            piece(before, 0, HALO), piece(j, HALO, HALO + bx), piece(after, HALO + bx, width)], axis=0)
        return jnp.dot(mx[k], rows, precision=HIGH)

    return jnp.stack([one(k) for k in range(slots)]).reshape(slots, -1)


def solution(mesh):
    return jax.shard_map(
        body,
        mesh=mesh,
        in_specs=(P("gx", "gy", "gz"), P(None, ("gx", "gy", "gz"))),
        out_specs=P(("gx", "gy", "gz"), None),
        check_vma=False,
    )
```

```python
import math

import jax
import jax.numpy as jnp
from jax import lax
from jax.experimental import pallas as pl
from jax.experimental.pallas import tpu as pltpu
from jax.sharding import PartitionSpec as P

G = 48
BOX = 68
HALO = 34
HIGH = lax.Precision.HIGH


def shift(array, axis, step):
    devices = lax.axis_size(axis)
    return lax.ppermute(array, axis, [(i, (i + step) % devices) for i in range(devices)])


def placed(start, cells, period, valid):
    place = cells - start[..., None]
    if period:
        place = jnp.mod(place, period)
    inside = jnp.logical_and(place >= 0, place < BOX)
    inside = jnp.logical_and(inside, valid[..., None])
    base = interp_values()
    index = jnp.where(inside, place, BOX)
    hot = (index[..., None, :] == jnp.arange(BOX, dtype=jnp.int32)[:, None]).astype(jnp.float32)
    return jnp.einsum("ax,...xe->...ae", base, hot, precision=lax.Precision.HIGHEST)


def interp_values():
    row_index = jnp.arange(G, dtype=jnp.int32)[:, None]
    col_index = jnp.arange(BOX, dtype=jnp.int32)[None, :]
    offset = row_index * BOX - col_index * G
    period = G * BOX
    summed = jnp.ones((G, BOX), jnp.float32)
    for harmonic in range(1, G // 2):
        phase_angle = jnp.mod(harmonic * offset, period).astype(jnp.float32)
        summed = summed + 2.0 * jnp.cos(2.0 * math.pi / period * phase_angle)
    return summed / BOX


LANES = 128
FOLD = LANES // HALO
STEPS = 4
BF = jnp.bfloat16
F32 = jnp.float32
FAR = -(1 << 20)


def split(value):
    high = value.astype(BF)
    return high, (value - high.astype(F32)).astype(BF)


def pack_kernel(pot, low, high):
    rows, by = pot.shape[1], pot.shape[2]
    lane = lax.broadcasted_iota(jnp.int32, (rows * by, LANES), 1)
    down = jnp.zeros((rows * by, LANES), F32)
    up = down
    for g in range(FOLD):
        v = pot[g].reshape(rows * by, LANES)
        mine = jnp.logical_and(lane >= g * HALO, lane < (g + 1) * HALO)
        down = jnp.where(mine, pltpu.roll(v, ((g + 1) * HALO) % LANES, 1), down)
        up = jnp.where(mine, pltpu.roll(v, g * HALO, 1) if g else v, up)
    low[...] = down.reshape(rows, by, LANES)
    high[...] = up.reshape(rows, by, LANES)


def pack(pot):
    fold, rows, by, bz = pot.shape
    step = rows // STEPS
    spec = pl.BlockSpec((step, by, LANES), lambda i: (i, 0, 0))
    shape = jax.ShapeDtypeStruct((rows, by, LANES), F32)
    return pl.pallas_call(
        pack_kernel,
        grid=(STEPS,),
        in_specs=[pl.BlockSpec((fold, step, by, LANES), lambda i: (0, i, 0, 0))],
        out_specs=[spec, spec],
        out_shape=[shape, shape],
        cost_estimate=pl.CostEstimate(flops=0, bytes_accessed=4 * pot.size * 2, transcendentals=0),
        name="pack_halos",
    )(pot)


def slab_kernel(ny, *refs):
    owns, lows, highs, out = refs[:ny], refs[ny:2 * ny], refs[2 * ny:3 * ny], refs[3 * ny]
    rows, by = owns[0].shape[1], owns[0].shape[2]
    pad = out.shape[2] // (2 * ny)
    half = ny * pad
    lane = lax.broadcasted_iota(jnp.int32, (pad, LANES), 1)
    blank = jnp.zeros((pad - by, LANES), F32)

    def full(v):
        return jnp.concatenate([v, blank], axis=0)

    for c in range(ny):
        for r in range(rows):
            up = full(highs[c][r])
            down = full(lows[c][r])
            for g in range(FOLD):
                first = full(owns[c][g, r])
                a = pltpu.roll(up, (-g * HALO) % LANES, 1) if g else up
                b = pltpu.roll(down, (HALO - g * HALO) % LANES, 1) if g != 1 else down
                second = jnp.where(lane < HALO, a, jnp.where(lane < 2 * HALO, b, 0.0))
                for side, v in ((0, first), (1, second)):
                    h, l = split(v)
                    cols = slice(side * LANES, (side + 1) * LANES)
                    out[g, r, c * pad:(c + 1) * pad, cols] = h
                    out[g, r, half + c * pad:half + (c + 1) * pad, cols] = l


def slabs(owns, lows, highs):
    ny = len(owns)
    fold, rows, by, bz = owns[0].shape
    pad = -(-by // 16) * 16
    step = rows // STEPS
    big = pl.BlockSpec((fold, step, by, LANES), lambda i: (0, i, 0, 0))
    small = pl.BlockSpec((step, by, LANES), lambda i: (i, 0, 0))
    return pl.pallas_call(
        lambda *refs: slab_kernel(ny, *refs),
        grid=(STEPS,),
        in_specs=[big] * ny + [small] * (2 * ny),
        out_specs=pl.BlockSpec((fold, step, 2 * ny * pad, 2 * LANES), lambda i: (0, i, 0, 0)),
        out_shape=jax.ShapeDtypeStruct((fold, rows, 2 * ny * pad, 2 * LANES), BF),
        cost_estimate=pl.CostEstimate(flops=0, bytes_accessed=16 * 1024 * 1024, transcendentals=0),
        name="build_slabs",
    )(*owns, *lows, *highs)


def contract_kernel(bx, yb, my, mz, out, lhs, wz, us):
    k = my.shape[2]
    for p in range(3):
        h, l = split(my[p])
        lhs[p, :G, :k] = h
        lhs[p, :G, k:] = h
        lhs[p, G:, :k] = l
        lhs[p, G:, k:] = jnp.zeros_like(l)
        h, l = split(mz[p])
        wz[p, 0] = h
        wz[p, 1] = l
    nl, nm = HALO // 8, bx // 8

    def row(p, x, s):
        r = jnp.dot(lhs[p], yb[x], preferred_element_type=F32)
        us[:, s, :] = r[:G] + r[G:]

    def finish(p):
        h, l = split(us[...].reshape(G * 8, us.shape[2]))
        dot = lambda a, b: jnp.dot(a, b, preferred_element_type=F32)
        return dot(h, wz[p, 0]) + dot(h, wz[p, 1]) + dot(l, wz[p, 0])

    def store(r, row0):
        for b in range(G):
            out[pl.ds(row0, 8), b * G:(b + 1) * G] = r[8 * b:8 * b + 8]

    def block(i, carry):
        p = (i >= nl).astype(jnp.int32) + (i >= nl + nm).astype(jnp.int32)
        x0 = jnp.where(p == 0, bx - HALO + 8 * i, jnp.where(p == 1, 8 * (i - nl), 8 * (i - nl - nm)))
        for s in range(8):
            row(p, x0 + s, s)
        store(finish(p), pl.multiple_of(8 * i, 8))
        return carry

    blocks = 2 * nl + nm
    lax.fori_loop(0, blocks, block, 0)
    tail = tail_rows(bx)
    for s, (p, x) in enumerate(tail):
        row(p, x, s)
    sub = lax.broadcasted_iota(jnp.int32, (G * 8, G), 0) % 8
    total = jnp.zeros((G * 8, G), F32)
    for p in range(3):
        places = [s for s, t in enumerate(tail) if t[0] == p]
        mine = jnp.logical_and(sub >= places[0], sub <= places[-1])
        total = jnp.where(mine, finish(p), total)
    store(total, 8 * blocks)


def tail_rows(bx):
    nl, nm = HALO // 8 * 8, bx // 8 * 8
    rows = [(0, bx - HALO + x) for x in range(nl, HALO)]
    rows += [(1, x) for x in range(nm, bx)]
    rows += [(2, x) for x in range(nl, HALO)]
    assert len(rows) == 8
    return rows


def row_order(bx):
    nl, nm = HALO // 8 * 8, bx // 8 * 8
    rows = [(0, bx - HALO + x) for x in range(nl)] + [(1, x) for x in range(nm)]
    return rows + [(2, x) for x in range(nl)] + tail_rows(bx)


def contract(bx, yb, my, mz):
    rows = len(row_order(bx))
    k = my.shape[2]
    width = yb.shape[2]
    return pl.pallas_call(
        lambda *refs: contract_kernel(bx, *refs),
        in_specs=[pl.BlockSpec(memory_space=pltpu.VMEM)] * 3,
        out_specs=pl.BlockSpec(memory_space=pltpu.VMEM),
        out_shape=jax.ShapeDtypeStruct((rows, G * G), F32),
        scratch_shapes=[
            pltpu.VMEM((3, 2 * G, 2 * k), BF),
            pltpu.VMEM((3, 2, width, G), BF),
            pltpu.VMEM((G, 8, width), F32),
        ],
        compiler_params=pltpu.CompilerParams(vmem_limit_bytes=40 * 1024 * 1024),
        cost_estimate=pl.CostEstimate(
            flops=6 * 10 ** 9, bytes_accessed=2 * yb.size + 4 * rows * G * G, transcendentals=0),
        name="contract_yz",
    )(yb, my, mz)


def body(potential, frag_root):
    bx, by, bz = potential.shape
    n = lax.axis_size("gx")
    ny = lax.axis_size("gy")
    nz = lax.axis_size("gz")
    ix, iy, iz = lax.axis_index("gx"), lax.axis_index("gy"), lax.axis_index("gz")
    total_x, total_y, total_z = bx * n, by * ny, bz * nz
    slots = frag_root.shape[1]

    folded = potential.reshape(FOLD, bx // FOLD, by, bz)
    low, high = pack(folded)
    low = shift(low, "gz", 1)
    high = shift(high, "gz", -1)
    owns = [folded] + [shift(folded, "gy", -j) for j in range(1, ny)]
    lows = [low] + [shift(low, "gy", -j) for j in range(1, ny)]
    highs = [high] + [shift(high, "gy", -j) for j in range(1, ny)]
    root = jnp.stack([frag_root] + [shift(frag_root, "gx", j) for j in range(1, n)])
    yb = slabs(owns, lows, highs)
    yb = yb.reshape(bx, yb.shape[2], yb.shape[3])

    anchor = jnp.mod(root[:, 0] + HALO, total_x) // bx
    start_y = jnp.mod(root[:, 1] - iy * by, total_y)
    start_z = jnp.mod(root[:, 2] + HALO - iz * bz, total_z)
    pad = -(-by // 16) * 16
    e = jnp.arange(ny * pad, dtype=jnp.int32)
    cells_y = e // pad * by + e % pad
    real_y = e % pad < by
    e = jnp.arange(2 * LANES, dtype=jnp.int32)
    cells_z = jnp.where(e < bz + HALO, e + HALO, jnp.where(e < bz + 2 * HALO, e - bz - HALO, FAR))
    delta = jnp.array([1, 0, -1], jnp.int32)
    hit = anchor[:, None, :] == jnp.mod(ix + delta, n)[None, :, None]
    valid = jnp.any(hit, axis=2)
    pick = lambda v: jnp.sum(jnp.where(hit, v[:, None, :], 0), axis=2)
    my = placed(pick(start_y), cells_y, total_y, valid)
    my = jnp.where(real_y, my, 0.0)
    mz = placed(pick(start_z), cells_z, None, valid).transpose(0, 1, 3, 2)

    order = [j for j in range(n) if j % 2] + [j for j in range(2, n, 2)]
    got = [None] * n
    for j in order:
        got[j] = shift(contract(bx, yb, my[j], mz[j]), "gx", -j)
    got[0] = contract(bx, yb, my[0], mz[0])

    mine = jnp.mod(frag_root[0] + HALO, total_x)
    slab = mine // bx
    rel = mine - slab * bx
    rows = row_order(bx)
    part = jnp.array([p for p, x in rows], jnp.int32)
    ext = jnp.array([x - (bx - HALO) if p == 0 else x + HALO + (p - 1) * bx for p, x in rows], jnp.int32)
    mx = placed(rel, ext, None, jnp.ones((slots,), bool))
    source = jnp.mod(slab[:, None] - ix + part[None, :] - 1, n)
    fields = None
    for j in [0] + order:
        m = jnp.where((source == j)[:, None, :], mx, 0.0).reshape(slots * G, -1)
        term = jnp.dot(m, got[j], precision=HIGH)
        fields = term if fields is None else fields + term
    return fields.reshape(slots, -1)


def solution(mesh):
    return jax.shard_map(
        body,
        mesh=mesh,
        in_specs=(P("gx", "gy", "gz"), P(None, ("gx", "gy", "gz"))),
        out_specs=P(("gx", "gy", "gz"), None),
        check_vma=False,
    )
```

```python
import math

import jax
import jax.numpy as jnp
from jax import lax
from jax.experimental import pallas as pl
from jax.experimental.pallas import tpu as pltpu
from jax.sharding import PartitionSpec as P

G = 48
BOX = 68
HALO = 34
HIGH = lax.Precision.HIGH


def shift(array, axis, step):
    devices = lax.axis_size(axis)
    return lax.ppermute(array, axis, [(i, (i + step) % devices) for i in range(devices)])


def placed(start, cells, period, valid):
    place = cells - start[..., None]
    if period:
        place = jnp.mod(place, period)
    inside = jnp.logical_and(place >= 0, place < BOX)
    inside = jnp.logical_and(inside, valid[..., None])
    base = interp_values()
    index = jnp.where(inside, place, BOX)
    hot = (index[..., None, :] == jnp.arange(BOX, dtype=jnp.int32)[:, None]).astype(jnp.float32)
    return jnp.einsum("ax,...xe->...ae", base, hot, precision=lax.Precision.HIGHEST)


def interp_values():
    row_index = jnp.arange(G, dtype=jnp.int32)[:, None]
    col_index = jnp.arange(BOX, dtype=jnp.int32)[None, :]
    offset = row_index * BOX - col_index * G
    period = G * BOX
    summed = jnp.ones((G, BOX), jnp.float32)
    for harmonic in range(1, G // 2):
        phase_angle = jnp.mod(harmonic * offset, period).astype(jnp.float32)
        summed = summed + 2.0 * jnp.cos(2.0 * math.pi / period * phase_angle)
    return summed / BOX


LANES = 128
FOLD = LANES // HALO
STEPS = 4
BF = jnp.bfloat16
F32 = jnp.float32
FAR = -(1 << 20)


def split(value):
    high = value.astype(BF)
    return high, (value - high.astype(F32)).astype(BF)


def pack_kernel(pot, low, high):
    rows, by = pot.shape[1], pot.shape[2]
    lane = lax.broadcasted_iota(jnp.int32, (rows * by, LANES), 1)
    down = jnp.zeros((rows * by, LANES), F32)
    up = down
    for g in range(FOLD):
        v = pot[g].reshape(rows * by, LANES)
        mine = jnp.logical_and(lane >= g * HALO, lane < (g + 1) * HALO)
        down = jnp.where(mine, pltpu.roll(v, ((g + 1) * HALO) % LANES, 1), down)
        up = jnp.where(mine, pltpu.roll(v, g * HALO, 1) if g else v, up)
    low[...] = down.reshape(rows, by, LANES)
    high[...] = up.reshape(rows, by, LANES)


def pack(pot):
    fold, rows, by, bz = pot.shape
    step = rows // STEPS
    spec = pl.BlockSpec((step, by, LANES), lambda i: (i, 0, 0))
    shape = jax.ShapeDtypeStruct((rows, by, LANES), F32)
    return pl.pallas_call(
        pack_kernel,
        grid=(STEPS,),
        in_specs=[pl.BlockSpec((fold, step, by, LANES), lambda i: (0, i, 0, 0))],
        out_specs=[spec, spec],
        out_shape=[shape, shape],
        cost_estimate=pl.CostEstimate(flops=0, bytes_accessed=4 * pot.size * 2, transcendentals=0),
        name="pack_halos",
    )(pot)


def slab_kernel(ny, *refs):
    owns, lows, highs, out = refs[:ny], refs[ny:2 * ny], refs[2 * ny:3 * ny], refs[3 * ny]
    rows, by = owns[0].shape[1], owns[0].shape[2]
    pad = out.shape[2] // (2 * ny)
    half = ny * pad
    lane = lax.broadcasted_iota(jnp.int32, (pad, LANES), 1)
    blank = jnp.zeros((pad - by, LANES), F32)

    def full(v):
        return jnp.concatenate([v, blank], axis=0)

    for c in range(ny):
        for r in range(rows):
            up = full(highs[c][r])
            down = full(lows[c][r])
            for g in range(FOLD):
                first = full(owns[c][g, r])
                a = pltpu.roll(up, (-g * HALO) % LANES, 1) if g else up
                b = pltpu.roll(down, (HALO - g * HALO) % LANES, 1) if g != 1 else down
                second = jnp.where(lane < HALO, a, jnp.where(lane < 2 * HALO, b, 0.0))
                for side, v in ((0, first), (1, second)):
                    h, l = split(v)
                    cols = slice(side * LANES, (side + 1) * LANES)
                    out[g, r, c * pad:(c + 1) * pad, cols] = h
                    out[g, r, half + c * pad:half + (c + 1) * pad, cols] = l


def slabs(owns, lows, highs):
    ny = len(owns)
    fold, rows, by, bz = owns[0].shape
    pad = -(-by // 16) * 16
    step = rows // STEPS
    big = pl.BlockSpec((fold, step, by, LANES), lambda i: (0, i, 0, 0))
    small = pl.BlockSpec((step, by, LANES), lambda i: (i, 0, 0))
    return pl.pallas_call(
        lambda *refs: slab_kernel(ny, *refs),
        grid=(STEPS,),
        in_specs=[big] * ny + [small] * (2 * ny),
        out_specs=pl.BlockSpec((fold, step, 2 * ny * pad, 2 * LANES), lambda i: (0, i, 0, 0)),
        out_shape=jax.ShapeDtypeStruct((fold, rows, 2 * ny * pad, 2 * LANES), BF),
        cost_estimate=pl.CostEstimate(flops=0, bytes_accessed=16 * 1024 * 1024, transcendentals=0),
        name="build_slabs",
    )(*owns, *lows, *highs)


def contract_kernel(bx, yb, my, mz, out, lhs, wz, us):
    k = my.shape[2]
    for p in range(3):
        h, l = split(my[p])
        lhs[p, :G, :k] = h
        lhs[p, :G, k:] = h
        lhs[p, G:, :k] = l
        lhs[p, G:, k:] = jnp.zeros_like(l)
        h, l = split(mz[p])
        wz[p, 0] = h
        wz[p, 1] = l
    nl, nm = HALO // 8, bx // 8

    def row(p, x, s):
        r = jnp.dot(lhs[p], yb[x], preferred_element_type=F32)
        us[:, s, :] = r[:G] + r[G:]

    def finish(p):
        h, l = split(us[...].reshape(G * 8, us.shape[2]))
        dot = lambda a, b: jnp.dot(a, b, preferred_element_type=F32)
        return dot(h, wz[p, 0]) + dot(h, wz[p, 1]) + dot(l, wz[p, 0])

    def store(r, row0):
        for b in range(G):
            out[pl.ds(row0, 8), b * G:(b + 1) * G] = r[8 * b:8 * b + 8]

    def block(i, carry):
        p = (i >= nl).astype(jnp.int32) + (i >= nl + nm).astype(jnp.int32)
        x0 = jnp.where(p == 0, bx - HALO + 8 * i, jnp.where(p == 1, 8 * (i - nl), 8 * (i - nl - nm)))
        for s in range(8):
            row(p, x0 + s, s)
        store(finish(p), pl.multiple_of(8 * i, 8))
        return carry

    blocks = 2 * nl + nm
    lax.fori_loop(0, blocks, block, 0)
    tail = tail_rows(bx)
    for s, (p, x) in enumerate(tail):
        row(p, x, s)
    sub = lax.broadcasted_iota(jnp.int32, (G * 8, G), 0) % 8
    total = jnp.zeros((G * 8, G), F32)
    for p in range(3):
        places = [s for s, t in enumerate(tail) if t[0] == p]
        mine = jnp.logical_and(sub >= places[0], sub <= places[-1])
        total = jnp.where(mine, finish(p), total)
    store(total, 8 * blocks)


def tail_rows(bx):
    nl, nm = HALO // 8 * 8, bx // 8 * 8
    rows = [(0, bx - HALO + x) for x in range(nl, HALO)]
    rows += [(1, x) for x in range(nm, bx)]
    rows += [(2, x) for x in range(nl, HALO)]
    assert len(rows) == 8
    return rows


def row_order(bx):
    nl, nm = HALO // 8 * 8, bx // 8 * 8
    rows = [(0, bx - HALO + x) for x in range(nl)] + [(1, x) for x in range(nm)]
    return rows + [(2, x) for x in range(nl)] + tail_rows(bx)


def contract(bx, yb, my, mz):
    rows = len(row_order(bx))
    k = my.shape[2]
    width = yb.shape[2]
    return pl.pallas_call(
        lambda *refs: contract_kernel(bx, *refs),
        in_specs=[pl.BlockSpec(memory_space=pltpu.VMEM)] * 3,
        out_specs=pl.BlockSpec(memory_space=pltpu.VMEM),
        out_shape=jax.ShapeDtypeStruct((rows, G * G), F32),
        scratch_shapes=[
            pltpu.VMEM((3, 2 * G, 2 * k), BF),
            pltpu.VMEM((3, 2, width, G), BF),
            pltpu.VMEM((G, 8, width), F32),
        ],
        compiler_params=pltpu.CompilerParams(vmem_limit_bytes=40 * 1024 * 1024),
        cost_estimate=pl.CostEstimate(
            flops=6 * 10 ** 9, bytes_accessed=2 * yb.size + 4 * rows * G * G, transcendentals=0),
        name="contract_yz",
    )(yb, my, mz)


def body(potential, frag_root):
    bx, by, bz = potential.shape
    n = lax.axis_size("gx")
    ny = lax.axis_size("gy")
    nz = lax.axis_size("gz")
    ix, iy, iz = lax.axis_index("gx"), lax.axis_index("gy"), lax.axis_index("gz")
    total_x, total_y, total_z = bx * n, by * ny, bz * nz
    slots = frag_root.shape[1]

    folded = potential.reshape(FOLD, bx // FOLD, by, bz)
    low, high = pack(folded)
    low = shift(low, "gz", 1)
    high = shift(high, "gz", -1)
    owns = [folded] + [shift(folded, "gy", -j) for j in range(1, ny)]
    lows = [low] + [shift(low, "gy", -j) for j in range(1, ny)]
    highs = [high] + [shift(high, "gy", -j) for j in range(1, ny)]
    root = jnp.stack([frag_root] + [shift(frag_root, "gx", j) for j in range(1, n)])
    yb = slabs(owns, lows, highs)
    yb = yb.reshape(bx, yb.shape[2], yb.shape[3])

    anchor = jnp.mod(root[:, 0] + HALO, total_x) // bx
    start_y = jnp.mod(root[:, 1] - iy * by, total_y)
    start_z = jnp.mod(root[:, 2] + HALO - iz * bz, total_z)
    pad = -(-by // 16) * 16
    e = jnp.arange(ny * pad, dtype=jnp.int32)
    cells_y = e // pad * by + e % pad
    real_y = e % pad < by
    e = jnp.arange(2 * LANES, dtype=jnp.int32)
    cells_z = jnp.where(e < bz + HALO, e + HALO, jnp.where(e < bz + 2 * HALO, e - bz - HALO, FAR))
    delta = jnp.array([1, 0, -1], jnp.int32)
    hit = anchor[:, None, :] == jnp.mod(ix + delta, n)[None, :, None]
    valid = jnp.any(hit, axis=2)
    pick = lambda v: jnp.sum(jnp.where(hit, v[:, None, :], 0), axis=2)
    my = placed(pick(start_y), cells_y, total_y, valid)
    my = jnp.where(real_y, my, 0.0)
    mz = placed(pick(start_z), cells_z, None, valid).transpose(0, 1, 3, 2)

    order = [j for j in range(2, n, 2)] + [j for j in range(n) if j % 2]
    got = [None] * n
    for j in order:
        got[j] = shift(contract(bx, yb, my[j], mz[j]), "gx", -j)
    got[0] = contract(bx, yb, my[0], mz[0])

    mine = jnp.mod(frag_root[0] + HALO, total_x)
    slab = mine // bx
    rel = mine - slab * bx
    rows = row_order(bx)
    part = jnp.array([p for p, x in rows], jnp.int32)
    ext = jnp.array([x - (bx - HALO) if p == 0 else x + HALO + (p - 1) * bx for p, x in rows], jnp.int32)
    mx = placed(rel, ext, None, jnp.ones((slots,), bool))
    source = jnp.mod(slab[:, None] - ix + part[None, :] - 1, n)
    fields = None
    for j in [0] + order:
        m = jnp.where((source == j)[:, None, :], mx, 0.0).reshape(slots * G, -1)
        term = jnp.dot(m, got[j], precision=HIGH)
        fields = term if fields is None else fields + term
    return fields.reshape(slots, -1)


def solution(mesh):
    return jax.shard_map(
        body,
        mesh=mesh,
        in_specs=(P("gx", "gy", "gz"), P(None, ("gx", "gy", "gz"))),
        out_specs=P(("gx", "gy", "gz"), None),
        check_vma=False,
    )
```
